32 devices in a mesh: dp: 8 (over z, x), mp: 4 (over y, core).
Axes of the slice: x: 2, y: 2, z: 4, core: 2. Of those that a mesh axis runs over, the one named last changes fastest.
Arguments:
- acts: bfloat16 [6144, 4, 1984], P('dp', 'mp'), may hold values from -6 to 6
- grads: bfloat16 [6144, 4, 1984], P('dp', 'mp'), may hold values from -0.21875 to 0.21875
- error: bfloat16 [8, 4, 1984, 1984], P('dp', 'mp'), may hold values from -4 to 4
- momentum: float32 [4, 1984, 1984], P('mp', 'dp'), may hold values from -4 to 4
- q_start: float32 [4, 1984, 128], P('mp'), may hold values from -0.125 to 0.125
Outputs:
- error_next: bfloat16 [8, 4, 1984, 1984], P('dp', 'mp')
- momentum_next: float32 [4, 1984, 1984], P('mp', 'dp')
- q_next: float32 [4, 1984, 128], P('mp')
The draws below stay inside these ranges and needn't reach their ends.
All inputs are finite; a program needn't handle non-finite values.
Results may differ from the reference program's by a relative error of at most 0.001.
Values sent between devices are 32-bit elements; how exact they have to be, the bound alone decides.
No kernel may reach another device: no remote copies, remote signals or barrier semaphores. Data moves between devices by JAX's collectives and lax.ppermute only.
A program may use at most 128 MiB of HBM per device.

```python
import jax
import jax.numpy as jnp
from jax import lax

D = 3968
RANK = 128
TOK_DEV = 768
TILE = 1984
TOKENS = 6144
N_DP = 8
N_MP = 4


def levels(stream_key, extent, cuts, smallest, high):
    loudness, own = 1.0, jax.random.fold_in(stream_key, 6)
    for dim, blocks in cuts:
        steps = jnp.exp(jax.random.uniform(jax.random.fold_in(own, dim), (blocks,), jnp.float32, smallest / len(cuts), high / len(cuts)))
        loudness = loudness * jnp.repeat(steps, extent[dim] // blocks).reshape([-1 if axis == dim else 1 for axis in range(len(extent))])
    return loudness


def noise(own_key, dims, deviation, reach, cuts=(), dtype=jnp.bfloat16):
    drawn = jax.random.normal(own_key, dims, jnp.float32) * deviation
    if len(cuts) > 0:
        drawn = levels(own_key, dims, cuts, -0.22, 0.18) * drawn
    return jnp.clip(drawn, min=-reach, max=reach).astype(dtype)


def setup_inputs(seed: int = 0) -> dict:
    key_list = jax.random.split(jax.random.key(seed), 6)
    acts = noise(key_list[0], (TOKENS, N_MP, TILE), 1.0, 6.0, ((0, 8), (1, 4)))
    grads = noise(key_list[1], (TOKENS, N_MP, TILE), TOK_DEV ** -0.5, 0.21875, ((0, 8), (1, 4)))
    error = noise(key_list[2], (N_DP, N_MP, TILE, TILE), 0.5, 4.0, ((0, 8), (1, 4)))
    momentum = noise(key_list[3], (N_MP, TILE, TILE), 0.5, 4.0, ((0, 4), (1, 8)), jnp.float32)
    q_start = noise(key_list[4], (N_MP, TILE, RANK), TILE ** -0.5, 0.125, ((0, 4),), jnp.float32)
    return {"acts": acts, "grads": grads, "error": error, "momentum": momentum, "q_start": q_start}


PRECISE = lax.Precision.HIGHEST

def merged_of(inputs, upstream, stored):
    local_grad = lax.dot_general(inputs.astype(jnp.float32), upstream.astype(jnp.float32), (((0,), (0,)), ((), ())), preferred_element_type=jnp.float32)
    return local_grad + stored.astype(jnp.float32)

def tile_step(pieces):
    acts_tile, grads_tile, error_tile, warm_start = pieces

    def add_left(carry, item):
        merged = merged_of(item[0], item[1], item[2])
        return (carry + jnp.dot(merged, warm_start, precision=PRECISE), None)
    left_full, unused = lax.scan(add_left, jnp.zeros((TILE, RANK), jnp.float32), (acts_tile, grads_tile, error_tile))
    gram_matrix = jnp.dot(left_full.T, left_full, precision=PRECISE)
    cholesky_low = jnp.linalg.cholesky(gram_matrix)
    ortho_basis = lax.linalg.triangular_solve(cholesky_low, left_full, left_side=False, lower=True, transpose_a=True)

    def add_right(carry, item):
        merged = merged_of(item[0], item[1], item[2])
        part_right = lax.dot_general(merged, ortho_basis, (((0,), (0,)), ((), ())), precision=PRECISE)
        return (carry + part_right, None)
    right_full, unused = lax.scan(add_right, jnp.zeros((TILE, RANK), jnp.float32), (acts_tile, grads_tile, error_tile))
    q_tile = right_full / N_DP
    decoded = jnp.dot(ortho_basis, q_tile.T, precision=PRECISE)

    def new_error(item):
        return (merged_of(item[0], item[1], item[2]) - decoded).astype(jnp.bfloat16)
    errors_out = lax.map(new_error, (acts_tile, grads_tile, error_tile))
    return (ortho_basis, q_tile, errors_out)

def reference(acts, grads, error, momentum, q_start):
    acts_tiles = acts.reshape(N_DP, TOK_DEV, N_MP, TILE).transpose(2, 0, 1, 3)
    grads_tiles = grads.reshape(N_DP, TOK_DEV, N_MP, TILE).transpose(2, 0, 1, 3)
    error_tiles = error.transpose(1, 0, 2, 3)
    ortho_all, q_next, errors_all = lax.map(tile_step, (acts_tiles, grads_tiles, error_tiles, q_start))
    norm_total = jnp.sum(q_next * q_next)
    rms_value = jnp.sqrt(norm_total / (D * D))
    decoded_all = jnp.einsum('tir,tjr->tij', ortho_all, q_next, precision=PRECISE)
    momentum_next = 0.9 * momentum + 0.1 * decoded_all / (rms_value + 1e-06)
    return (errors_all.transpose(1, 0, 2, 3), momentum_next, q_next)
```

```python
import functools

import jax
import jax.numpy as jnp
from jax import lax
from jax.experimental import pallas as pl
from jax.experimental.pallas import tpu as pltpu
from jax.sharding import PartitionSpec as P


F32, BF16 = jnp.float32, jnp.bfloat16
PRECISE = lax.Precision.HIGHEST
NN = (((1,), (0,)), ((), ()))
NT = (((1,), (1,)), ((), ()))
TN = (((0,), (0,)), ((), ()))
VMEM_LIMIT = 48 * 2**20


def dot(a, b, dims, precision=None):
    return lax.dot_general(a, b, dims, precision=precision, preferred_element_type=F32)


def quarter(tile):
    return tile // 4


def lane_quarter(tile):
    return pl.cdiv(tile, 512) * 128


def split(x):
    high = x.astype(BF16)
    return high, (x - high.astype(F32)).astype(BF16)


def cost(flops, nbytes):
    return pl.CostEstimate(flops=int(flops), bytes_accessed=int(nbytes), transcendentals=0)


def sequential(axes=1):
    return pltpu.CompilerParams(
        dimension_semantics=("arbitrary",) * axes, vmem_limit_bytes=VMEM_LIMIT
    )


def store_split(ref, x):
    rows = x.shape[0]
    high, low = split(x)
    ref[:rows] = high
    ref[rows:] = low


def left_first_kernel(where_ref, q_ref, grads_ref, acts_ref, error_ref, out_ref, q_split, mid_split):
    rank = out_ref.shape[1]

    @pl.when(pl.program_id(0) == 0)
    def _():
        high, low = split(q_ref[...])
        q_split[:, :rank] = high
        q_split[:, rank:] = low
        mid = dot(q_split[...], grads_ref[...], TN)
        store_split(mid_split, mid[:rank] + mid[rank:])

    left_rest_kernel(where_ref, q_split, mid_split, acts_ref, error_ref, out_ref)


def left_rest_kernel(where_ref, q_split, mid_split, acts_ref, error_ref, out_ref):
    rank = out_ref.shape[1]
    both = dot(error_ref[...], q_split[...], NN) + dot(acts_ref[...], mid_split[...], NT)
    out_ref[...] = both[:, :rank] + both[:, rank:]


def left_first(where, q, grads_t, acts_t, error):
    tile, tokens = acts_t.shape
    rank, blocks, block_rows = q.shape[1], where.shape[0], quarter(tile) // 2
    whole = lambda i, w: (0, 0)
    return pl.pallas_call(
        left_first_kernel,
        grid_spec=pltpu.PrefetchScalarGridSpec(
            num_scalar_prefetch=1,
            grid=(blocks,),
            in_specs=[
                pl.BlockSpec((tile, rank), whole),
                pl.BlockSpec((tile, tokens), whole),
                pl.BlockSpec((block_rows, tokens), lambda i, w: (w[i], 0)),
                pl.BlockSpec((block_rows, tile), lambda i, w: (w[i], 0)),
            ],
            out_specs=[
                pl.BlockSpec((block_rows, rank), lambda i, w: (i, 0)),
                pl.BlockSpec((tile, 2 * rank), whole),
                pl.BlockSpec((2 * rank, tokens), whole),
            ],
        ),
        out_shape=[
            jax.ShapeDtypeStruct((blocks * block_rows, rank), F32),
            jax.ShapeDtypeStruct((tile, 2 * rank), BF16),
            jax.ShapeDtypeStruct((2 * rank, tokens), BF16),
        ],
        cost_estimate=cost(4 * rank * tile * (tile // 2 + 2 * tokens), tile * (tile + 3 * tokens)),
        compiler_params=sequential(),
        name="left_first",
    )(where, q, grads_t, acts_t, error)


def left_rest(where, q_split, mid_split, acts_t, error):
    tile, tokens = acts_t.shape
    rank, blocks, block_rows = q_split.shape[1] // 2, where.shape[0], quarter(tile) // 2
    whole = lambda i, w: (0, 0)
    return pl.pallas_call(
        left_rest_kernel,
        grid_spec=pltpu.PrefetchScalarGridSpec(
            num_scalar_prefetch=1,
            grid=(blocks,),
            in_specs=[
                pl.BlockSpec((tile, 2 * rank), whole),
                pl.BlockSpec((2 * rank, tokens), whole),
                pl.BlockSpec((block_rows, tokens), lambda i, w: (w[i], 0)),
                pl.BlockSpec((block_rows, tile), lambda i, w: (w[i], 0)),
            ],
            out_specs=pl.BlockSpec((block_rows, rank), lambda i, w: (i, 0)),
        ),
        out_shape=jax.ShapeDtypeStruct((blocks * block_rows, rank), F32),
        cost_estimate=cost(2 * rank * tile * (tile + tokens), tile * (tile + tokens)),
        compiler_params=sequential(),
        name="left_rest",
    )(where, q_split, mid_split, acts_t, error)


def right_step(left_ref, acts_ref, error_ref, acc_ref, mid_ref, left_split):
    rank = acc_ref.shape[0]
    store_split(left_split, left_ref[...].T)
    both = dot(left_split[...], error_ref[...], NN)
    acc_ref[...] += both[:rank] + both[rank:]
    both = dot(left_split[...], acts_ref[...], NN)
    mid_ref[...] += both[:rank] + both[rank:]


def right_first_kernel(where_ref, left_ref, acts_ref, error_ref, acc_ref, mid_ref, left_split):
    step = pl.program_id(0)

    @pl.when(step == 0)
    def _():
        acc_ref[...] = jnp.zeros_like(acc_ref)
        mid_ref[...] = jnp.zeros_like(mid_ref)

    right_step(left_ref, acts_ref, error_ref, acc_ref, mid_ref, left_split)


def right_last_kernel(
    where_ref, left_ref, acts_ref, error_ref, grads_ref, acc_in, mid_in, out_ref, acc, mid, left_split, mid_split
):
    step = pl.program_id(0)
    rank = acc.shape[0]

    @pl.when(step == 0)
    def _():
        acc[...] = acc_in[...]
        mid[...] = mid_in[...]

    right_step(left_ref, acts_ref, error_ref, acc, mid, left_split)

    @pl.when(step == pl.num_programs(0) - 1)
    def _():
        store_split(mid_split, mid[...])
        both = dot(mid_split[...], grads_ref[...], NT)
        out_ref[...] = (acc[...] + both[:rank] + both[rank:]).T


def right_first(where, left, acts_t, error):
    tile, tokens = acts_t.shape
    rank, blocks, part_rows = left.shape[1], where.shape[0], quarter(tile)
    whole = lambda i, w: (0, 0)
    return pl.pallas_call(
        right_first_kernel,
        grid_spec=pltpu.PrefetchScalarGridSpec(
            num_scalar_prefetch=1,
            grid=(blocks,),
            in_specs=[
                pl.BlockSpec((part_rows, rank), lambda i, w: (i, 0)),
                pl.BlockSpec((part_rows, tokens), lambda i, w: (w[i], 0)),
                pl.BlockSpec((part_rows, tile), lambda i, w: (w[i], 0)),
            ],
            out_specs=[pl.BlockSpec((rank, tile), whole), pl.BlockSpec((rank, tokens), whole)],
            scratch_shapes=[pltpu.VMEM((2 * rank, part_rows), BF16)],
        ),
        out_shape=[
            jax.ShapeDtypeStruct((rank, tile), F32),
            jax.ShapeDtypeStruct((rank, tokens), F32),
        ],
        cost_estimate=cost(2 * rank * tile * (tile + tokens), tile * (tile + tokens)),
        compiler_params=sequential(),
        name="right_first",
    )(where, left, acts_t, error)


def right_last(where, left, acts_t, error, grads_t, acc, mid):
    tile, tokens = acts_t.shape
    rank, blocks, part_rows = left.shape[1], where.shape[0], quarter(tile)
    whole = lambda i, w: (0, 0)
    return pl.pallas_call(
        right_last_kernel,
        grid_spec=pltpu.PrefetchScalarGridSpec(
            num_scalar_prefetch=1,
            grid=(blocks,),
            in_specs=[
                pl.BlockSpec((part_rows, rank), lambda i, w: (i, 0)),
                pl.BlockSpec((part_rows, tokens), lambda i, w: (w[i], 0)),
                pl.BlockSpec((part_rows, tile), lambda i, w: (w[i], 0)),
                pl.BlockSpec((tile, tokens), whole),
                pl.BlockSpec((rank, tile), whole),
                pl.BlockSpec((rank, tokens), whole),
            ],
            out_specs=pl.BlockSpec((tile, rank), whole),
            scratch_shapes=[
                pltpu.VMEM((rank, tile), F32),
                pltpu.VMEM((rank, tokens), F32),
                pltpu.VMEM((2 * rank, part_rows), BF16),
                pltpu.VMEM((2 * rank, tokens), BF16),
            ],
        ),
        out_shape=jax.ShapeDtypeStruct((tile, rank), F32),
        cost_estimate=cost(4 * rank * tile * (tile // 2 + 2 * tokens), tile * (tile + 3 * tokens)),
        compiler_params=sequential(),
        name="right_last",
    )(where, left, acts_t, error, grads_t, acc, mid)


def gram_kernel(left_ref, out_ref):
    turned = left_ref[...].T
    out_ref[...] = dot(turned, turned, NT, PRECISE)


def gram_product(left):
    rank = left.shape[1]
    return pl.pallas_call(
        gram_kernel,
        out_shape=jax.ShapeDtypeStruct((rank, rank), F32),
        cost_estimate=cost(100 * rank * rank * left.shape[0], 4 * rank * left.shape[0]),
        name="gram",
    )(left)


def rsqrt(x):
    r = lax.rsqrt(x)
    return r * (1.5 - 0.5 * x * r * r)


def inverse_kernel(gram_ref, out_ref):
    n = gram_ref.shape[0]
    groups = n // 8
    whole = [gram_ref[8 * h : 8 * h + 8] for h in range(groups)]
    lanes = lax.broadcasted_iota(jnp.int32, (8, n), 1)
    rows = lax.broadcasted_iota(jnp.int32, (8, n), 0)
    inverse = [jnp.where(lanes == rows + 8 * h, 1.0, 0.0) for h in range(groups)]
    for j in range(0, n, 2):
        g, i = j // 8, j % 8
        first = [jnp.broadcast_to(whole[h][:, j : j + 1], (8, n)) for h in range(g, groups)]
        second = [jnp.broadcast_to(whole[h][:, j + 1 : j + 2], (8, n)) for h in range(g, groups)]
        r1 = rsqrt(first[0][i : i + 1])
        l21 = first[0][i + 1 : i + 2] * r1
        r2 = rsqrt(second[0][i + 1 : i + 2] - l21 * l21)
        row1 = whole[g][i : i + 1] * r1
        row2 = (whole[g][i + 1 : i + 2] - l21 * row1) * r2
        out1 = inverse[g][i : i + 1] * r1
        out2 = (inverse[g][i + 1 : i + 2] - l21 * out1) * r2
        for h in range(g, groups):
            m1 = first[h - g] * r1
            m2 = (second[h - g] - l21 * m1) * r2
            update = inverse[h] - m1 * out1 - m2 * out2
            if h == g:
                update = jnp.where(rows > i + 1, update, inverse[h])
                update = jnp.where(rows == i, out1, jnp.where(rows == i + 1, out2, update))
            inverse[h] = update
            if 8 * h + 8 > j + 2:
                whole[h] = whole[h] - m1 * row1 - m2 * row2
        if i == 6:
            out_ref[8 * g : 8 * g + 8] = inverse[g]


def inverse_factor(gram):
    n = gram.shape[0]
    return pl.pallas_call(
        inverse_kernel,
        out_shape=jax.ShapeDtypeStruct((n, n), F32),
        cost_estimate=cost(8e9, 8 * n * n),
        name="inverse_factor",
    )(gram)


def ortho_kernel(left_ref, inverse_ref, terms_ref):
    y = dot(left_ref[...], inverse_ref[...], NT, PRECISE)
    rank = y.shape[1]
    high, low = split(y)
    terms_ref[:, :rank] = high
    terms_ref[:, rank : 2 * rank] = high
    terms_ref[:, 2 * rank :] = low


def ortho_terms_of(left, inverse):
    padded, rank = left.shape
    rows = padded // 4
    return pl.pallas_call(
        ortho_kernel,
        grid=(padded // rows,),
        in_specs=[
            pl.BlockSpec((rows, rank), lambda i: (i, 0)),
            pl.BlockSpec((rank, rank), lambda i: (0, 0)),
        ],
        out_specs=pl.BlockSpec((rows, 3 * rank), lambda i: (i, 0)),
        out_shape=jax.ShapeDtypeStruct((padded, 3 * rank), BF16),
        cost_estimate=cost(100 * rank * rank * padded, 12 * rank * padded),
        compiler_params=sequential(),
        name="ortho",
    )(left, inverse)


def error_kernel(scale, right_ref, inverse_ref, acts_ref, grads_ref, ortho_ref, error_ref, out_ref, q_ref, square_ref, q_terms):
    rank = q_ref.shape[1]

    @pl.when(pl.program_id(0) == 0)
    def _():
        q = dot(right_ref[...], inverse_ref[...], NT, PRECISE) * scale
        q_ref[...] = q
        square_ref[...] = jnp.full(square_ref.shape, jnp.sum(q * q), F32)
        high, low = split(q)
        q_terms[:, :rank] = high
        q_terms[:, rank : 2 * rank] = low
        q_terms[:, 2 * rank :] = high

    merged = dot(acts_ref[...], grads_ref[...], NT) + error_ref[...].astype(F32)
    out_ref[...] = (merged - dot(ortho_ref[...], q_terms[...], NT)).astype(out_ref.dtype)


def error_update(right, inverse, acts_t, grads_t, ortho_terms, error, scale):
    tile, tokens = acts_t.shape
    rank, terms = right.shape[1], ortho_terms.shape[1]
    part_rows = quarter(tile)
    whole = lambda i: (0, 0)
    return pl.pallas_call(
        functools.partial(error_kernel, scale),
        grid=(tile // part_rows,),
        in_specs=[
            pl.BlockSpec((tile, rank), whole),
            pl.BlockSpec((rank, rank), whole),
            pl.BlockSpec((part_rows, tokens), lambda i: (i, 0)),
            pl.BlockSpec((tile, tokens), whole),
            pl.BlockSpec((part_rows, terms), lambda i: (i, 0)),
            pl.BlockSpec((part_rows, tile), lambda i: (i, 0)),
        ],
        out_specs=[
            pl.BlockSpec((part_rows, tile), lambda i: (i, 0)),
            pl.BlockSpec((tile, rank), whole),
            pl.BlockSpec((8, 128), whole),
        ],
        out_shape=[
            jax.ShapeDtypeStruct(error.shape, BF16),
            jax.ShapeDtypeStruct((tile, rank), F32),
            jax.ShapeDtypeStruct((8, 128), F32),
        ],
        scratch_shapes=[pltpu.VMEM((tile, terms), BF16)],
        cost_estimate=cost(2 * tile * tile * (tokens + terms), 4 * tile * tile),
        compiler_params=sequential(),
        name="error_update",
    )(right, inverse, acts_t, grads_t, ortho_terms, error)


def momentum_kernel(scale_ref, ortho_ref, q_ref, momentum_ref, out_ref):
    rank = q_ref.shape[1]
    high, low = split(q_ref[...])
    update = dot(ortho_ref[:, :rank], high, NT)
    update += dot(ortho_ref[:, :rank], low, NT)
    update += dot(ortho_ref[:, 2 * rank :], high, NT)
    out_ref[...] = 0.9 * momentum_ref[...] + update * scale_ref[0, 0]


def momentum_update(scale, ortho_own, q, momentum):
    rows, tile = momentum.shape
    terms = ortho_own.shape[1]
    return pl.pallas_call(
        momentum_kernel,
        out_shape=jax.ShapeDtypeStruct(momentum.shape, F32),
        cost_estimate=cost(2 * rows * tile * terms, 8 * rows * tile),
        name="momentum_update",
    )(scale, ortho_own, q, momentum)


def partner(value, axis, bit):
    pairs = [(i, i ^ bit) for i in range(lax.axis_size(axis))]
    return lax.ppermute(value, axis, pairs)


def exchange_orders(axis):
    size = lax.axis_size(axis)
    bits = [1 << i for i in range(size.bit_length() - 1)]
    return bits, bits[1::-1] + bits[2:]


def place(axis, bit):
    return (lax.axis_index(axis) // bit) % 2


def halve(parts, orders, axis, stages):
    for stage in stages:
        sent = []
        for j, part in enumerate(parts):
            bit, rows = orders[j][stage], part.shape[0] // 2
            send = lax.dynamic_slice_in_dim(part, (1 - place(axis, bit)) * rows, rows, 0)
            sent.append(partner(send, axis, bit))
        for j, part in enumerate(parts):
            bit, rows = orders[j][stage], part.shape[0] // 2
            parts[j] = lax.dynamic_slice_in_dim(part, place(axis, bit) * rows, rows, 0) + sent[j]
    return parts


def in_order(mine, one, other):
    return jnp.concatenate([jnp.where(mine == 0, one, other), jnp.where(mine == 0, other, one)], 0)


def grow(parts, orders, axis, stages):
    for stage in stages:
        others = [partner(part, axis, orders[j][stage]) for j, part in enumerate(parts)]
        parts = [in_order(place(axis, orders[j][stage]), part, others[j]) for j, part in enumerate(parts)]
    return parts


def small_sum(value, axis):
    size = lax.axis_size(axis)
    bit = 1
    while bit < size:
        value = value + partner(value, axis, bit)
        bit *= 2
    return value


def per_device(acts, grads, error, momentum, q_start):
    acts_t, grads_t = acts[:, 0, :].T, grads[:, 0, :].T
    stored, warm_start = error[0, 0], q_start[0]
    tile, rank = warm_start.shape
    replicas = lax.axis_size("dp")
    part_rows = quarter(tile)
    right_half = 2 * lane_quarter(tile)
    owned_rows = momentum.shape[1]
    orders = exchange_orders("dp")
    last = len(orders[0]) - 1
    middle = range(1, last)
    first_place = [place("dp", orders[j][0]) for j in range(2)]
    known = jnp.stack([first_place[0], 2 + first_place[1]]).astype(jnp.int32)
    other = jnp.stack([1 - first_place[0], 3 - first_place[1]]).astype(jnp.int32)
    fine = lambda blocks: jnp.stack([2 * blocks, 2 * blocks + 1], 1).reshape(-1)

    with jax.named_scope("left"):
        send, q_split, mid_split = left_first(fine(other), warm_start, grads_t, acts_t, stored)
        came = [partner(send[j * part_rows : (j + 1) * part_rows], "dp", orders[j][0]) for j in range(2)]
        keep = left_rest(fine(known), q_split, mid_split, acts_t, stored)
        parts = [keep[j * part_rows : (j + 1) * part_rows] + came[j] for j in range(2)]
        parts = halve(parts, orders, "dp", middle)
        parts = [part + partner(part, "dp", orders[j][last]) for j, part in enumerate(parts)]
        parts = grow(parts, orders, "dp", reversed(middle))
        came = [partner(parts[j], "dp", orders[j][0]) for j in range(2)]

    with jax.named_scope("right"):
        acc, mid = right_first(known, jnp.concatenate(parts, 0), acts_t, stored)
        right = right_last(other, jnp.concatenate(came, 0), acts_t, stored, grads_t, acc, mid)
        left = jnp.concatenate([in_order(first_place[j], parts[j], came[j]) for j in range(2)], 0)
        parts = halve([right[:right_half], right[right_half:]], orders, "dp", range(1))
        left, parts = lax.optimization_barrier((left, parts))
        gram = gram_product(left)
        parts = halve(parts, orders, "dp", middle)
        gram, parts = lax.optimization_barrier((gram, parts))
        inverse = inverse_factor(gram)
        parts = [part + partner(part, "dp", orders[j][last]) for j, part in enumerate(parts)]
        inverse, parts = lax.optimization_barrier((inverse, parts))
        parts = grow(parts, orders, "dp", reversed(middle))
        came = [partner(parts[j], "dp", orders[j][0]) for j in range(2)]
        right = jnp.concatenate([in_order(first_place[j], parts[j], came[j]) for j in range(2)], 0)

    with jax.named_scope("tail"):
        ortho = ortho_terms_of(left, inverse)
        error_next, q_tile, square = error_update(
            right, inverse, acts_t, grads_t, ortho, stored, 1.0 / replicas
        )
        norm = small_sum(square, "mp")
        total = tile * tile * lax.axis_size("mp")
        scale = 0.1 / (jnp.sqrt(norm / total) + 1e-06)
        ortho_own = lax.dynamic_slice_in_dim(ortho, lax.axis_index("dp") * owned_rows, owned_rows, 0)
        momentum_next = momentum_update(scale, ortho_own, q_tile, momentum[0])
    return (error_next[None, None], momentum_next[None], q_tile[None])


def solution(mesh):
    in_specs = (
        P("dp", "mp", None),
        P("dp", "mp", None),
        P("dp", "mp", None, None),
        P("mp", "dp", None),
        P("mp", None, None),
    )
    out_specs = (P("dp", "mp", None, None), P("mp", "dp", None), P("mp", None, None))
    return jax.shard_map(
        per_device, mesh=mesh, in_specs=in_specs, out_specs=out_specs, check_vma=False
    )
```

```python
import functools

import jax
import jax.numpy as jnp
from jax import lax
from jax.experimental import pallas as pl
from jax.experimental.pallas import tpu as pltpu
from jax.sharding import PartitionSpec as P


F32, BF16 = jnp.float32, jnp.bfloat16
PRECISE = lax.Precision.HIGHEST
NN = (((1,), (0,)), ((), ()))
NT = (((1,), (1,)), ((), ()))
TN = (((0,), (0,)), ((), ()))
VMEM_LIMIT = 48 * 2**20
FIRST_LIMIT = 60 * 1024 * 2**10


def dot(a, b, dims, precision=None):
    return lax.dot_general(a, b, dims, precision=precision, preferred_element_type=F32)


def quarter(tile):
    return tile // 4


def lane_quarter(tile):
    return pl.cdiv(tile, 512) * 128


def split(x):
    high = x.astype(BF16)
    return high, (x - high.astype(F32)).astype(BF16)


def cost(flops, nbytes):
    return pl.CostEstimate(flops=int(flops), bytes_accessed=int(nbytes), transcendentals=0)


def sequential(limit=VMEM_LIMIT):
    return pltpu.CompilerParams(dimension_semantics=("arbitrary",), vmem_limit_bytes=limit)


def store_split(ref, x):
    rows = x.shape[0]
    high, low = split(x)
    ref[:rows] = high
    ref[rows:] = low


def left_first_kernel(blocks, where_ref, q_ref, grads_ref, *refs):
    acts_refs, error_ref = refs[:blocks], refs[blocks]
    out_a, out_b, q_split, mid_split, acc, mid_acc = refs[blocks + 1 :]
    rank = out_a.shape[1]
    step = pl.program_id(0)
    rows, chunk = error_ref.shape[0], grads_ref.shape[0]

    @pl.when(step == 0)
    def _():
        high, low = split(q_ref[...])
        q_split[:, :rank] = high
        q_split[:, rank:] = low
        mid_acc[...] = jnp.zeros_like(mid_acc)

    both = dot(error_ref[...], q_split[...], NN)
    acc[pl.ds(pl.multiple_of(step * rows, 8), rows)] = both[:, :rank] + both[:, rank:]
    q_rows = q_split[pl.ds(pl.multiple_of(step * chunk, 16), chunk)]
    mid_acc[...] += dot(q_rows, grads_ref[...], TN)

    @pl.when(step == blocks - 1)
    def _():
        store_split(mid_split, mid_acc[:rank] + mid_acc[rank:])
        for k, acts_ref in enumerate(acts_refs):
            both = dot(acts_ref[...], mid_split[...], NT)
            value = acc[k * rows : (k + 1) * rows] + both[:, :rank] + both[:, rank:]
            if k < blocks // 2:
                out_a[k * rows : (k + 1) * rows] = value
            else:
                out_b[(k - blocks // 2) * rows : (k + 1 - blocks // 2) * rows] = value


def left_rest_kernel(blocks, where_ref, q_split, mid_split, acts_ref, error_ref, out_a, out_b):
    rank = out_a.shape[1]
    step = pl.program_id(0)
    rows = error_ref.shape[0]
    both = dot(error_ref[...], q_split[...], NN) + dot(acts_ref[...], mid_split[...], NT)
    value = both[:, :rank] + both[:, rank:]
    spot = pl.ds(pl.multiple_of(lax.rem(step, blocks // 2) * rows, 8), rows)

    @pl.when(step < blocks // 2)
    def _():
        out_a[spot] = value

    @pl.when(step >= blocks // 2)
    def _():
        out_b[spot] = value


def left_first(where, q, grads_t, acts_t, error):
    tile, tokens = acts_t.shape
    rank, blocks, block_rows = q.shape[1], where.shape[0], quarter(tile) // 2
    whole = lambda i, w: (0, 0)
    chunk = tile // blocks
    acts_specs = [
        pl.BlockSpec((block_rows, tokens), functools.partial(lambda k, i, w: (w[k], 0), k))
        for k in range(blocks)
    ]
    return pl.pallas_call(
        functools.partial(left_first_kernel, blocks),
        grid_spec=pltpu.PrefetchScalarGridSpec(
            num_scalar_prefetch=1,
            grid=(blocks,),
            in_specs=[
                pl.BlockSpec((tile, rank), whole),
                pl.BlockSpec((chunk, tokens), lambda i, w: (i, 0)),
                *acts_specs,
                pl.BlockSpec((block_rows, tile), lambda i, w: (w[i], 0)),
            ],
            out_specs=[
                pl.BlockSpec((blocks // 2 * block_rows, rank), whole),
                pl.BlockSpec((blocks // 2 * block_rows, rank), whole),
                pl.BlockSpec((tile, 2 * rank), whole),
                pl.BlockSpec((2 * rank, tokens), whole),
            ],
            scratch_shapes=[
                pltpu.VMEM((blocks * block_rows, rank), F32),
                pltpu.VMEM((2 * rank, tokens), F32),
            ],
        ),
        out_shape=[
            jax.ShapeDtypeStruct((blocks // 2 * block_rows, rank), F32),
            jax.ShapeDtypeStruct((blocks // 2 * block_rows, rank), F32),
            jax.ShapeDtypeStruct((tile, 2 * rank), BF16),
            jax.ShapeDtypeStruct((2 * rank, tokens), BF16),
        ],
        cost_estimate=cost(4 * rank * tile * (tile // 2 + 2 * tokens), tile * (tile + 3 * tokens)),
        compiler_params=sequential(limit=FIRST_LIMIT),
        name="left_first",
    )(where, q, grads_t, *[acts_t] * blocks, error)


def left_rest(where, q_split, mid_split, acts_t, error):
    tile, tokens = acts_t.shape
    rank, blocks, block_rows = q_split.shape[1] // 2, where.shape[0], quarter(tile) // 2
    whole = lambda i, w: (0, 0)
    half = jax.ShapeDtypeStruct((blocks // 2 * block_rows, rank), F32)
    return pl.pallas_call(
        functools.partial(left_rest_kernel, blocks),
        grid_spec=pltpu.PrefetchScalarGridSpec(
            num_scalar_prefetch=1,
            grid=(blocks,),
            in_specs=[
                pl.BlockSpec((tile, 2 * rank), whole),
                pl.BlockSpec((2 * rank, tokens), whole),
                pl.BlockSpec((block_rows, tokens), lambda i, w: (w[i], 0)),
                pl.BlockSpec((block_rows, tile), lambda i, w: (w[i], 0)),
            ],
            out_specs=[pl.BlockSpec(half.shape, whole)] * 2,
        ),
        out_shape=[half, half],
        cost_estimate=cost(2 * rank * tile * (tile + tokens), tile * (tile + tokens)),
        compiler_params=sequential(limit=16 * 2**20),
        name="left_rest",
    )(where, q_split, mid_split, acts_t, error)


def right_step(left_ref, acts_ref, error_ref, acc_ref, mid_ref, left_split):
    rank = acc_ref.shape[0]
    store_split(left_split, left_ref[...].T)
    both = dot(left_split[...], error_ref[...], NN)
    acc_ref[...] += both[:rank] + both[rank:]
    both = dot(left_split[...], acts_ref[...], NN)
    mid_ref[...] += both[:rank] + both[rank:]


def right_first_kernel(where_ref, left_ref, acts_ref, error_ref, acc_ref, mid_ref, left_split):
    step = pl.program_id(0)

    @pl.when(step == 0)
    def _():
        acc_ref[...] = jnp.zeros_like(acc_ref)
        mid_ref[...] = jnp.zeros_like(mid_ref)

    right_step(left_ref, acts_ref, error_ref, acc_ref, mid_ref, left_split)


def right_last_kernel(
    where_ref, left_ref, acts_ref, error_ref, grads_ref, acc_in, mid_in, out_ref, acc, mid, left_split, mid_split
):
    step = pl.program_id(0)
    rank = acc.shape[0]

    @pl.when(step == 0)
    def _():
        acc[...] = acc_in[...]
        mid[...] = mid_in[...]

    right_step(left_ref, acts_ref, error_ref, acc, mid, left_split)

    @pl.when(step == pl.num_programs(0) - 1)
    def _():
        store_split(mid_split, mid[...])
        both = dot(mid_split[...], grads_ref[...], NT)
        out_ref[...] = (acc[...] + both[:rank] + both[rank:]).T


def right_first(where, left, acts_t, error):
    tile, tokens = acts_t.shape
    rank, blocks, part_rows = left.shape[1], where.shape[0], quarter(tile)
    whole = lambda i, w: (0, 0)
    return pl.pallas_call(
        right_first_kernel,
        grid_spec=pltpu.PrefetchScalarGridSpec(
            num_scalar_prefetch=1,
            grid=(blocks,),
            in_specs=[
                pl.BlockSpec((part_rows, rank), lambda i, w: (i, 0)),
                pl.BlockSpec((part_rows, tokens), lambda i, w: (w[i], 0)),
                pl.BlockSpec((part_rows, tile), lambda i, w: (w[i], 0)),
            ],
            out_specs=[pl.BlockSpec((rank, tile), whole), pl.BlockSpec((rank, tokens), whole)],
            scratch_shapes=[pltpu.VMEM((2 * rank, part_rows), BF16)],
        ),
        out_shape=[
            jax.ShapeDtypeStruct((rank, tile), F32),
            jax.ShapeDtypeStruct((rank, tokens), F32),
        ],
        cost_estimate=cost(2 * rank * tile * (tile + tokens), tile * (tile + tokens)),
        compiler_params=sequential(limit=24 * 2**20),
        name="right_first",
    )(where, left, acts_t, error)


def right_last(where, left, acts_t, error, grads_t, acc, mid):
    tile, tokens = acts_t.shape
    rank, blocks, part_rows = left.shape[1], where.shape[0], quarter(tile)
    whole = lambda i, w: (0, 0)
    return pl.pallas_call(
        right_last_kernel,
        grid_spec=pltpu.PrefetchScalarGridSpec(
            num_scalar_prefetch=1,
            grid=(blocks,),
            in_specs=[
                pl.BlockSpec((part_rows, rank), lambda i, w: (i, 0)),
                pl.BlockSpec((part_rows, tokens), lambda i, w: (w[i], 0)),
                pl.BlockSpec((part_rows, tile), lambda i, w: (w[i], 0)),
                pl.BlockSpec((tile, tokens), whole),
                pl.BlockSpec((rank, tile), whole),
                pl.BlockSpec((rank, tokens), whole),
            ],
            out_specs=pl.BlockSpec((tile, rank), whole),
            scratch_shapes=[
                pltpu.VMEM((rank, tile), F32),
                pltpu.VMEM((rank, tokens), F32),
                pltpu.VMEM((2 * rank, part_rows), BF16),
                pltpu.VMEM((2 * rank, tokens), BF16),
            ],
        ),
        out_shape=jax.ShapeDtypeStruct((tile, rank), F32),
        cost_estimate=cost(4 * rank * tile * (tile // 2 + 2 * tokens), tile * (tile + 3 * tokens)),
        compiler_params=sequential(limit=32 * 2**20),
        name="right_last",
    )(where, left, acts_t, error, grads_t, acc, mid)


def gram_kernel(left_ref, out_ref):
    turned = left_ref[...].T
    out_ref[...] = dot(turned, turned, NT, PRECISE)


def gram_product(left):
    rank = left.shape[1]
    return pl.pallas_call(
        gram_kernel,
        out_shape=jax.ShapeDtypeStruct((rank, rank), F32),
        cost_estimate=cost(100 * rank * rank * left.shape[0], 4 * rank * left.shape[0]),
        compiler_params=pltpu.CompilerParams(vmem_limit_bytes=8 * 2**20),
        name="gram",
    )(left)


def rsqrt(x):
    r = lax.rsqrt(x)
    return r * (1.5 - 0.5 * x * r * r)


def inverse_kernel(gram_ref, out_ref):
    n = gram_ref.shape[0]
    groups = n // 8
    whole = [gram_ref[8 * h : 8 * h + 8] for h in range(groups)]
    lanes = lax.broadcasted_iota(jnp.int32, (8, n), 1)
    rows = lax.broadcasted_iota(jnp.int32, (8, n), 0)
    inverse = [jnp.where(lanes == rows + 8 * h, 1.0, 0.0) for h in range(groups)]
    for j in range(0, n, 2):
        g, i = j // 8, j % 8
        first = [jnp.broadcast_to(whole[h][:, j : j + 1], (8, n)) for h in range(g, groups)]
        second = [jnp.broadcast_to(whole[h][:, j + 1 : j + 2], (8, n)) for h in range(g, groups)]
        r1 = rsqrt(first[0][i : i + 1])
        l21 = first[0][i + 1 : i + 2] * r1
        r2 = rsqrt(second[0][i + 1 : i + 2] - l21 * l21)
        row1 = whole[g][i : i + 1] * r1
        row2 = (whole[g][i + 1 : i + 2] - l21 * row1) * r2
        out1 = inverse[g][i : i + 1] * r1
        out2 = (inverse[g][i + 1 : i + 2] - l21 * out1) * r2
        for h in range(g, groups):
            m1 = first[h - g] * r1
            m2 = (second[h - g] - l21 * m1) * r2
            update = inverse[h] - m1 * out1 - m2 * out2
            if h == g:
                update = jnp.where(rows > i + 1, update, inverse[h])
                update = jnp.where(rows == i, out1, jnp.where(rows == i + 1, out2, update))
            inverse[h] = update
            if 8 * h + 8 > j + 2:
                whole[h] = whole[h] - m1 * row1 - m2 * row2
        if i == 6:
            out_ref[8 * g : 8 * g + 8] = inverse[g]


def inverse_factor(gram):
    n = gram.shape[0]
    return pl.pallas_call(
        inverse_kernel,
        out_shape=jax.ShapeDtypeStruct((n, n), F32),
        cost_estimate=cost(8e9, 8 * n * n),
        compiler_params=pltpu.CompilerParams(vmem_limit_bytes=8 * 2**20),
        name="inverse_factor",
    )(gram)


def ortho_kernel(left_ref, inverse_ref, terms_ref):
    y = dot(left_ref[...], inverse_ref[...], NT, PRECISE)
    rank = y.shape[1]
    high, low = split(y)
    terms_ref[:, :rank] = high
    terms_ref[:, rank : 2 * rank] = high
    terms_ref[:, 2 * rank :] = low


def ortho_terms_of(left, inverse):
    padded, rank = left.shape
    rows = padded // 4
    return pl.pallas_call(
        ortho_kernel,
        grid=(padded // rows,),
        in_specs=[
            pl.BlockSpec((rows, rank), lambda i: (i, 0)),
            pl.BlockSpec((rank, rank), lambda i: (0, 0)),
        ],
        out_specs=pl.BlockSpec((rows, 3 * rank), lambda i: (i, 0)),
        out_shape=jax.ShapeDtypeStruct((padded, 3 * rank), BF16),
        cost_estimate=cost(100 * rank * rank * padded, 12 * rank * padded),
        compiler_params=sequential(limit=12 * 2**20),
        name="ortho",
    )(left, inverse)


def q_kernel(scale, right_ref, inverse_ref, q_ref, terms_ref, square_ref):
    rank = q_ref.shape[1]
    q = dot(right_ref[...], inverse_ref[...], NT, PRECISE) * scale
    q_ref[...] = q
    high, low = split(q)
    rows = q.shape[0]
    terms_ref[:rows, :rank] = high
    terms_ref[:rows, rank : 2 * rank] = low
    terms_ref[:rows, 2 * rank :] = high
    if rows < terms_ref.shape[0]:
        terms_ref[rows:] = jnp.zeros((terms_ref.shape[0] - rows, 3 * rank), BF16)
    square_ref[...] = jnp.full(square_ref.shape, jnp.sum(q * q), F32)


def q_of(right, inverse, scale):
    tile, rank = right.shape
    return pl.pallas_call(
        functools.partial(q_kernel, scale),
        out_shape=[
            jax.ShapeDtypeStruct((tile, rank), F32),
            jax.ShapeDtypeStruct((4 * lane_quarter(tile), 3 * rank), BF16),
            jax.ShapeDtypeStruct((8, 128), F32),
        ],
        cost_estimate=cost(12 * rank * rank * tile, 12 * rank * tile),
        compiler_params=pltpu.CompilerParams(vmem_limit_bytes=20 * 2**20),
        name="q_of",
    )(right, inverse)


def error_kernel(acts_ref, grads_ref, ortho_ref, q_ref, error_ref, out_ref):
    merged = dot(acts_ref[...], grads_ref[...], NT) + error_ref[...].astype(F32)
    out_ref[...] = (merged - dot(ortho_ref[...], q_ref[: grads_ref.shape[0]], NT)).astype(out_ref.dtype)


def error_update(acts_t, grads_t, ortho_terms, q_terms, error):
    tile, tokens = acts_t.shape
    terms = ortho_terms.shape[1]
    part_rows = quarter(tile)
    whole = lambda i: (0, 0)
    return pl.pallas_call(
        error_kernel,
        grid=(tile // part_rows,),
        in_specs=[
            pl.BlockSpec((part_rows, tokens), lambda i: (i, 0)),
            pl.BlockSpec((tile, tokens), whole),
            pl.BlockSpec((part_rows, terms), lambda i: (i, 0)),
            pl.BlockSpec(q_terms.shape, whole),
            pl.BlockSpec((part_rows, tile), lambda i: (i, 0)),
        ],
        out_specs=pl.BlockSpec((part_rows, tile), lambda i: (i, 0)),
        out_shape=jax.ShapeDtypeStruct(error.shape, BF16),
        cost_estimate=cost(2 * tile * tile * (tokens + terms), 4 * tile * tile),
        compiler_params=sequential(),
        name="error_update",
    )(acts_t, grads_t, ortho_terms, q_terms, error)


def momentum_kernel(scale_ref, ortho_ref, q_ref, momentum_ref, out_ref):
    update = dot(ortho_ref[...], q_ref[...], NT)
    out_ref[...] = 0.9 * momentum_ref[...] + update * scale_ref[0, 0]


def momentum_update(scale, ortho_own, q_terms, momentum):
    rows, tile = momentum.shape
    terms = ortho_own.shape[1]
    cols = lane_quarter(tile)
    return pl.pallas_call(
        momentum_kernel,
        grid=(pl.cdiv(tile, cols),),
        in_specs=[
            pl.BlockSpec((8, 128), lambda j: (0, 0)),
            pl.BlockSpec((rows, terms), lambda j: (0, 0)),
            pl.BlockSpec((cols, terms), lambda j: (j, 0)),
            pl.BlockSpec((rows, cols), lambda j: (0, j)),
        ],
        out_specs=pl.BlockSpec((rows, cols), lambda j: (0, j)),
        out_shape=jax.ShapeDtypeStruct(momentum.shape, F32),
        cost_estimate=cost(2 * rows * tile * terms, 8 * rows * tile),
        compiler_params=sequential(limit=16 * 2**20),
        name="momentum_update",
    )(scale, ortho_own, q_terms, momentum)


def partner(value, axis, bit):
    pairs = [(i, i ^ bit) for i in range(lax.axis_size(axis))]
    return lax.ppermute(value, axis, pairs)


def exchange_orders(axis):
    size = lax.axis_size(axis)
    bits = [1 << i for i in range(size.bit_length() - 1)]
    return bits, bits[1::-1] + bits[2:]


def place(axis, bit):
    return (lax.axis_index(axis) // bit) % 2


def halve(parts, orders, axis, stages):
    for stage in stages:
        sent = []
        for j, part in enumerate(parts):
            bit, rows = orders[j][stage], part.shape[0] // 2
            send = lax.dynamic_slice_in_dim(part, (1 - place(axis, bit)) * rows, rows, 0)
            sent.append(partner(send, axis, bit))
        for j, part in enumerate(parts):
            bit, rows = orders[j][stage], part.shape[0] // 2
            parts[j] = lax.dynamic_slice_in_dim(part, place(axis, bit) * rows, rows, 0) + sent[j]
    return parts


def in_order(mine, one, other):
    return jnp.concatenate([jnp.where(mine == 0, one, other), jnp.where(mine == 0, other, one)], 0)


def grow(parts, orders, axis, stages):
    for stage in stages:
        others = [partner(part, axis, orders[j][stage]) for j, part in enumerate(parts)]
        parts = [in_order(place(axis, orders[j][stage]), part, others[j]) for j, part in enumerate(parts)]
    return parts


def others_of(value, axis):
    size = lax.axis_size(axis)
    return [lax.ppermute(value, axis, [(i, (i + k) % size) for i in range(size)]) for k in range(1, size)]


def per_device(acts, grads, error, momentum, q_start):
    acts_t, grads_t = acts[:, 0, :].T, grads[:, 0, :].T
    stored, warm_start = error[0, 0], q_start[0]
    tile, rank = warm_start.shape
    replicas = lax.axis_size("dp")
    part_rows = quarter(tile)
    right_half = 2 * lane_quarter(tile)
    owned_rows = momentum.shape[1]
    orders = exchange_orders("dp")
    last = len(orders[0]) - 1
    middle = range(1, last)
    first_place = [place("dp", orders[j][0]) for j in range(2)]
    known = jnp.stack([first_place[0], 2 + first_place[1]]).astype(jnp.int32)
    other = jnp.stack([1 - first_place[0], 3 - first_place[1]]).astype(jnp.int32)
    fine = lambda blocks: jnp.stack([2 * blocks, 2 * blocks + 1], 1).reshape(-1)

    with jax.named_scope("left"):
        *send, q_split, mid_split = left_first(fine(other), warm_start, grads_t, acts_t, stored)
        came = [partner(send[j], "dp", orders[j][0]) for j in range(2)]
        keep = left_rest(fine(known), q_split, mid_split, acts_t, stored)
        parts = [keep[j] + came[j] for j in range(2)]
        parts = halve(parts, orders, "dp", middle)
        parts = [part + partner(part, "dp", orders[j][last]) for j, part in enumerate(parts)]
        parts = grow(parts, orders, "dp", reversed(middle))
        came = [partner(parts[j], "dp", orders[j][0]) for j in range(2)]

    with jax.named_scope("right"):
        acc, mid = right_first(known, jnp.concatenate(parts, 0), acts_t, stored)
        right = right_last(other, jnp.concatenate(came, 0), acts_t, stored, grads_t, acc, mid)
        left = jnp.concatenate([in_order(first_place[j], parts[j], came[j]) for j in range(2)], 0)
        parts = halve([right[:right_half], right[right_half:]], orders, "dp", range(1))
        parts = halve(parts, orders, "dp", middle)
        left, parts = lax.optimization_barrier((left, parts))
        gram = gram_product(left)
        inverse = inverse_factor(gram)
        parts = [part + partner(part, "dp", orders[j][last]) for j, part in enumerate(parts)]
        inverse, parts = lax.optimization_barrier((inverse, parts))
        parts = grow(parts, orders, "dp", reversed(middle))
        left, parts = lax.optimization_barrier((left, parts))
        came = [partner(parts[j], "dp", orders[j][0]) for j in range(2)]
        right = jnp.concatenate([in_order(first_place[j], parts[j], came[j]) for j in range(2)], 0)

    with jax.named_scope("tail"):
        ortho = ortho_terms_of(left, inverse)
        q_tile, q_terms, square = q_of(right, inverse, 1.0 / replicas)
        others = others_of(square, "mp")
        error_next = error_update(acts_t, grads_t, ortho, q_terms, stored)
        norm = sum(others, square)
        total = tile * tile * lax.axis_size("mp")
        scale = 0.1 / (jnp.sqrt(norm / total) + 1e-06)
        ortho_own = lax.dynamic_slice_in_dim(ortho, lax.axis_index("dp") * owned_rows, owned_rows, 0)
        momentum_next = momentum_update(scale, ortho_own, q_terms, momentum[0])
    return (error_next[None, None], momentum_next[None], q_tile[None])


def solution(mesh):
    in_specs = (
        P("dp", "mp", None),
        P("dp", "mp", None),
        P("dp", "mp", None, None),
        P("mp", "dp", None),
        P("mp", None, None),
    )
    out_specs = (P("dp", "mp", None, None), P("mp", "dp", None), P("mp", None, None))
    return jax.shard_map(
        per_device, mesh=mesh, in_specs=in_specs, out_specs=out_specs, check_vma=False
    )
```
